32 devices in a mesh: gx: 2 (over x), gy: 4 (over z), wa: 4 (over y, core).
Axes of the slice: x: 2, y: 2, z: 4, core: 2. Of those that a mesh axis runs over, the one named last changes fastest.
Arguments:
- velocity: float32 [3, 64, 256, 512], P(None, 'gx', 'gy', 'wa'), may hold values from -70 to 70, as said below
- lengths: int32 [2, 4, 4, 2048], P('gx', 'gy', 'wa'), may hold values from 16 to 128
- destinations: int32 [2, 4, 4, 2048, 1], P('gx', 'gy', 'wa'), may hold values from 0 to 7; in each aligned block of 2048 rows (0 to 2047, 2048 to 4095, ..., all dimensions but the last counted through in order) at most 512 rows name the same one
Outputs:
- received: float32 [8, 4, 3, 8, 512, 128], P(('gx', 'gy'), 'wa')
The draws below stay inside these ranges and needn't reach their ends.
Inputs may be any that keep to these rules, and one draw needn't show every extreme that they name: `velocity`: finite values; the amplitude varies over the grid. `destinations`: in every draw no device sends more than 512 blocks to one writer, and some device sends exactly 512 to one writer.
All inputs are finite; a program needn't handle non-finite values.
Results may differ from the reference program's by a relative error of at most 0.0003.
Values sent between devices are 32-bit elements; how exact they have to be, the bound alone decides.
A program may use at most 128 MiB of HBM per device.

```python
import math
import jax
import jax.numpy as jnp
import numpy as np
from jax import lax

CX = 32
CY = 64
CZ = 128
COMP = 3
BY = 8
BZ = 16
COEF = 128
NBLK = 2048
WRITERS = 8
CAP = 512
NX = 64
NY = 256
NZ = 512
N_GX = 2
N_GY = 4
N_WA = 4


def draw_velocity(key, part):
    xs = jnp.arange(NX, dtype=jnp.float32)[:, None, None] / NX
    ys = jnp.arange(NY, dtype=jnp.float32)[None, :, None] / NY
    noise = jax.random.truncated_normal(key, -6.0, 6.0, (COMP, NX, NY, NZ), jnp.float32)
    amplitude = jnp.exp(jnp.log(10.0) * 0.5 * (xs + ys))
    return amplitude * noise


def place_ends(entries, rng, least, high):
    shape = entries.shape
    spot = [jax.random.randint(jax.random.fold_in(rng, axis), (), 0, shape[axis]) for axis in range(len(shape))]
    entries = entries.at[tuple(spot)].set(least)
    longest = shape.index(max(shape))
    spot[longest] = (spot[longest] + 1) % shape[longest]
    return entries.at[tuple(spot)].set(high)


def shared_out(own_key, own, number, rows, number_of, top, bound, skew):
    sequence = jax.random.permutation(own_key, number_of)
    crowded, usual = load_shares(number_of, rows * top, bound, skew, True), load_shares(number_of, rows * top, bound, skew, False)
    places = jnp.arange(number_of)

    def named(tallies, turn):
        used = int((tallies > 0).sum())
        fixed = max(1, used // 4)
        passed = fixed + (places - fixed + turn * (used - fixed)) % max(1, number_of - fixed)
        return jnp.zeros((number_of,), jnp.int32).at[sequence[jnp.where(places < fixed, places, passed)]].set(jnp.asarray(tallies, jnp.int32))

    tallies = jnp.where(number % 4 == 0, named(crowded, number // 4), named(usual, number - number // 4 - 1))
    mixed = jax.random.permutation(jax.random.fold_in(own, 3), number_of)
    giver, receiver = mixed[0:number_of // 2 * 2:2], mixed[1:number_of // 2 * 2:2]
    room = jnp.minimum(tallies[giver] - 1, bound - tallies[receiver]) // 2
    room = jnp.where((giver == sequence[0]) | (receiver == sequence[0]) | (tallies[receiver] == 0), 0, jnp.maximum(room, 0))
    passed = jax.random.randint(jax.random.fold_in(own, 4), (number_of // 2,), 0, 1 << 20) % (room + 1)
    tallies = tallies.at[giver].add(-passed).at[receiver].add(passed)
    members = jnp.searchsorted(jnp.cumsum(tallies), jnp.arange(rows * top), side="right").astype(jnp.int32)
    grid = members.reshape(top, rows).T
    grid = grid[jax.random.permutation(jax.random.fold_in(own, 1), rows)]
    turn = jax.random.randint(jax.random.fold_in(own, 2), (rows, 1), 0, top)
    return jnp.take_along_axis(grid, (jnp.arange(top)[None, :] + turn) % top, axis=1)


def load_shares(count, total, reach, lean, full):
    weights = [(1 << 20) // math.isqrt(standing ** lean) + 1 for standing in range(1, count + 1)]
    largest = reach if full else min(reach, max(-(-total // count), total * weights[0] // sum(weights)))
    least = 1 if total - largest >= count - 1 else 0
    given, spare = [largest] + [least] * (count - 1), total - largest - least * (count - 1)
    while spare > 0:
        free = [i for i in range(1, count) if given[i] < largest] or [i for i in range(1, count) if given[i] < reach]
        pool, budget = sum([weights[i] for i in free]), spare
        for i in free:
            more = min(reach - given[i], max(1, budget * weights[i] // pool), spare)
            given[i] = given[i] + more
            spare = spare - more
    return np.array(given)


def setup_inputs(seed: int = 0) -> dict:
    key_list = jax.random.split(jax.random.key(seed), 4)
    velocity = draw_velocity(jax.random.fold_in(key_list[3], 71), 0)
    lengths = place_ends(jax.random.randint(key_list[1], (N_GX, N_GY, N_WA, NBLK), 16, COEF + 1), jax.random.fold_in(key_list[1], 1), 16, COEF).astype(jnp.int32)
    destinations_keys = jax.random.split(jax.random.fold_in(key_list[2], 1), N_GX * N_GY * N_WA * NBLK // NBLK)
    destinations_turns = jax.random.permutation(jax.random.fold_in(key_list[2], 3), N_GX * N_GY * N_WA * NBLK // NBLK)
    destinations = jax.vmap(lambda own, number: shared_out(jax.random.fold_in(key_list[2], 2), own, number, NBLK, WRITERS, 1, CAP, 2))(destinations_keys, destinations_turns).reshape((N_GX, N_GY, N_WA, NBLK, 1))
    return dict(velocity=velocity, lengths=lengths, destinations=destinations)


def dct_table(count):
    freqs = jnp.arange(count, dtype=jnp.float32)[:, None]
    points = jnp.arange(count, dtype=jnp.float32)[None, :]
    table = jnp.cos(jnp.pi * (points + 0.5) * freqs / count) * jnp.sqrt(2.0 / count)
    return jnp.where(freqs == 0.0, table * jnp.sqrt(0.5), table)

def curl_field(padded):

    def along_x(component):
        return (padded[component, 2:, 1:-1, 1:-1] - padded[component, :-2, 1:-1, 1:-1]) * 0.5

    def along_y(component):
        return (padded[component, 1:-1, 2:, 1:-1] - padded[component, 1:-1, :-2, 1:-1]) * 0.5

    def along_z(component):
        return (padded[component, 1:-1, 1:-1, 2:] - padded[component, 1:-1, 1:-1, :-2]) * 0.5
    first = along_y(2) - along_z(1)
    second = along_z(0) - along_x(2)
    third = along_x(1) - along_y(0)
    return jnp.stack([first, second, third])

def place_blocks(scaled, lens, targets):
    onehot = (targets[:, None] == jnp.arange(WRITERS, dtype=jnp.int32)[None, :]).astype(jnp.int32)
    before = jnp.cumsum(onehot, axis=0) - onehot
    ranking = lax.optimization_barrier(jnp.sum(before * onehot, axis=1))
    slot_index = (targets * CAP + ranking).astype(jnp.int32)
    buffer = jnp.zeros((WRITERS * CAP, COMP, COEF), jnp.float32)
    buffer = buffer.at[slot_index].set(scaled)
    return buffer.reshape(WRITERS, CAP, COMP, COEF)

def reference(velocity, lengths, destinations):
    padded = jnp.pad(velocity, ((0, 0), (1, 1), (1, 1), (1, 1)), mode='wrap')
    curl = curl_field(padded)
    total = jnp.sum(curl * curl)
    rms = jnp.sqrt(total / (COMP * NX * NY * NZ) + 1e-06)
    kron_table = jnp.kron(dct_table(BY), dct_table(BZ))
    grouped = curl.reshape(COMP, N_GX, CX, N_GY, CY // BY, BY, N_WA, CZ // BZ, BZ)
    grouped = grouped.transpose(1, 3, 6, 2, 4, 7, 0, 5, 8)
    blocks = grouped.reshape(-1, COEF)
    coeffs = jnp.dot(blocks, kron_table.T, precision=lax.Precision.HIGHEST, preferred_element_type=jnp.float32)
    coeffs = coeffs.reshape(N_GX * N_GY * N_WA, NBLK, COMP, COEF)
    freqs = jnp.arange(COEF, dtype=jnp.int32)
    lens = lengths.reshape(N_GX * N_GY * N_WA, NBLK)
    keep = (freqs[None, None, None, :] < lens[:, :, None, None]).astype(jnp.float32)
    scaled = coeffs * keep / rms
    targets = destinations.reshape(N_GX * N_GY * N_WA, NBLK)
    buffers = jax.vmap(place_blocks)(scaled, lens, targets)
    buffers = buffers.reshape(WRITERS, N_WA, WRITERS, CAP, COMP, COEF)
    return buffers.transpose(2, 1, 4, 0, 3, 5)
```

```python
import functools

import jax
import jax.numpy as jnp
import numpy as np
from jax import lax
from jax.experimental import pallas as pl
from jax.experimental.pallas import tpu as pltpu
from jax.sharding import PartitionSpec as P

BY = 8
BZ = 16
MESH = pl.DeviceIdType.MESH


def dct_table(count):
    freqs, points = np.arange(count)[:, None], np.arange(count)[None, :]
    table = np.cos(np.pi * (points + 0.5) * freqs / count) * np.sqrt(2.0 / count)
    return np.where(freqs == 0, table * np.sqrt(0.5), table)


def split_table():
    kron = np.kron(dct_table(BY), dct_table(BZ)).T.astype(np.float32)
    high = kron.astype(jnp.bfloat16)
    low = (kron - high.astype(np.float32)).astype(jnp.bfloat16)
    return np.block([[high, low], [high, np.zeros_like(low)]]).astype(jnp.bfloat16)


def faces(array, axis):
    peers = lax.axis_size(axis)
    up = [(i, (i + 1) % peers) for i in range(peers)]
    down = [(j, i) for i, j in up]
    first, last = array
    return lax.ppermute(last, axis, up), lax.ppermute(first, axis, down)


def slot_kernel(writers, capacity, targets, slots):
    t = targets[...]
    rows, lanes = t.shape
    shape = (lanes, lanes)
    upper = (
        lax.broadcasted_iota(jnp.int32, shape, 0) < lax.broadcasted_iota(jnp.int32, shape, 1)
    ).astype(jnp.float32).astype(jnp.bfloat16)
    square = (rows, rows)
    lower = (
        lax.broadcasted_iota(jnp.int32, square, 1) < lax.broadcasted_iota(jnp.int32, square, 0)
    ).astype(jnp.float32).astype(jnp.bfloat16)

    def body(w, acc):
        mine = t == w
        ones = mine.astype(jnp.float32).astype(jnp.bfloat16)
        inner = jnp.dot(ones, upper, preferred_element_type=jnp.float32)
        before = jnp.dot(lower, ones, preferred_element_type=jnp.float32)
        rank = inner + jnp.sum(before, axis=1, keepdims=True)
        return jnp.where(mine, w * capacity + rank.astype(jnp.int32), acc)

    slots[...] = lax.fori_loop(0, writers, body, jnp.zeros_like(t))


def block_rows(plane):
    cells_y, cells_z = plane.shape
    tiles = plane.reshape(cells_y // BY, BY, cells_z)
    sub = lax.broadcasted_iota(jnp.int32, tiles.shape, 1)
    group = lax.broadcasted_iota(jnp.int32, tiles.shape, 2) // BZ
    k = 1
    while k < BY:
        s_bit, g_bit = (sub & k) != 0, (group & k) != 0
        fwd = pltpu.roll(pltpu.roll(tiles, BY - k, 1), k * BZ, 2)
        back = pltpu.roll(pltpu.roll(tiles, k, 1), cells_z - k * BZ, 2)
        tiles = jnp.where(s_bit == g_bit, tiles, jnp.where(g_bit, fwd, back))
        k *= 2
    return tiles.reshape(cells_y, cells_z)


def blocks_kernel(
    slots, lens, vel, xb, xa, yb, ya, zb, za, table, out, squares, coeffs
):
    comps, cells_x, cells_y, cells_z = vel.shape
    nblk = coeffs.shape[1]
    per_plane = nblk // cells_x
    rows = out.shape[0] // comps
    width = out.shape[1]
    row = lax.broadcasted_iota(jnp.int32, (cells_y, cells_z), 0)
    lane = lax.broadcasted_iota(jnp.int32, (cells_y, cells_z), 1)
    chunk = 128

    def clear(i, _):
        out[pl.ds(pl.multiple_of(i * chunk, chunk), chunk), :] = jnp.zeros(
            (chunk, width), jnp.float32
        )
        return 0

    lax.fori_loop(0, out.shape[0] // chunk, clear, 0)

    def plane(x, acc):
        u, v, w = vel[0, x], vel[1, x], vel[2, x]

        def along_x(comp):
            nxt = jnp.where(
                x == cells_x - 1, xa[comp - 1], vel[comp, jnp.minimum(x + 1, cells_x - 1)]
            )
            prv = jnp.where(x == 0, xb[comp - 1], vel[comp, jnp.maximum(x - 1, 0)])
            return (nxt - prv) * 0.5

        def along_y(f, face):
            nxt = jnp.where(
                row == cells_y - 1, ya[face, pl.ds(x, 1), :], pltpu.roll(f, cells_y - 1, 0)
            )
            prv = jnp.where(row == 0, yb[face, pl.ds(x, 1), :], pltpu.roll(f, 1, 0))
            return (nxt - prv) * 0.5

        def along_z(f, face):
            after = pltpu.roll(za[face], cells_z - 1 - x, 1)
            before = pltpu.roll(zb[face], lax.rem(cells_z - x, cells_z), 1)
            nxt = jnp.where(lane == cells_z - 1, after, pltpu.roll(f, cells_z - 1, 1))
            prv = jnp.where(lane == 0, before, pltpu.roll(f, 1, 1))
            return (nxt - prv) * 0.5

        curl = (
            along_y(w, 1) - along_z(v, 1),
            along_z(u, 0) - along_x(2),
            along_x(1) - along_y(u, 0),
        )
        for c in curl:
            acc = acc + jnp.sum((c * c).reshape(cells_y // 8, 8, cells_z), axis=0)
        flat = jnp.concatenate([block_rows(c) for c in curl], axis=0)
        high = flat.astype(jnp.bfloat16)
        low = (flat - high.astype(jnp.float32)).astype(jnp.bfloat16)
        both = jnp.dot(
            jnp.concatenate([high, low], axis=1), table[...], preferred_element_type=jnp.float32
        )
        result = both[:, :width] + both[:, width:]
        start = pl.multiple_of(x * per_plane, 8)
        for c in range(comps):
            coeffs[c, pl.ds(start, per_plane), :] = result[c * per_plane : (c + 1) * per_plane]
        return acc

    squares[...] = lax.fori_loop(0, cells_x, plane, jnp.zeros((8, cells_z), jnp.float32))
    freqs = lax.broadcasted_iota(jnp.int32, (1, width), 1)
    group = 8

    def place(j, _):
        for k in range(group):
            i = j * group + k
            slot, keep = slots[i], freqs < lens[i]
            for c in range(comps):
                out[pl.ds(c * rows + slot, 1), :] = jnp.where(
                    keep, coeffs[c, pl.ds(i, 1), :], 0.0
                )
        return 0

    lax.fori_loop(0, nblk // group, place, 0)


def exchange_kernel(n_x, n_y, send, recv, send_sem, recv_sem):
    a, b = lax.axis_index("gx"), lax.axis_index("gy")
    c = lax.axis_index("wa")
    me = a * n_y + b
    offsets = [(i, j) for i in range(n_x) for j in range(n_y) if i or j]
    offsets.sort(key=lambda o: (bool(o[0]) and bool(o[1]), min(o[1], n_y - o[1])))
    barrier = pltpu.get_barrier_semaphore()
    peers = [(lax.rem(a + i, n_x), lax.rem(b + j, n_y)) for i, j in offsets]
    for pa, pb in peers:
        pl.semaphore_signal(barrier, inc=1, device_id=(pa, pb, c), device_id_type=MESH)
    pl.semaphore_wait(barrier, len(peers))
    copies = []
    for k, (pa, pb) in enumerate(peers):
        copy = pltpu.make_async_remote_copy(
            src_ref=send.at[:, pa * n_y + pb],
            dst_ref=recv.at[:, me],
            send_sem=send_sem.at[k],
            recv_sem=recv_sem.at[k],
            device_id=(pa, pb, c),
            device_id_type=MESH,
        )
        copy.start()
        copies.append(copy)
    for copy in copies:
        copy.wait()


def scale_kernel(every, me, squares, recv, send, out):
    total = jnp.sum(squares[...], keepdims=True)
    scale = 1.0 / jnp.sqrt(total / every + 1e-06)
    own = pl.program_id(1) == me[0]

    @pl.when(own)
    def _():
        out[...] = send[...] * scale[None, None]

    @pl.when(jnp.logical_not(own))
    def _():
        out[...] = recv[...] * scale[None, None]


def local(velocity, lengths, destinations):
    n_x, n_y, n_z = lax.axis_size("gx"), lax.axis_size("gy"), lax.axis_size("wa")
    comps, cells_x, cells_y, cells_z = velocity.shape
    width = BY * BZ
    nblk = cells_x * cells_y * cells_z // width
    writers = n_x * n_y
    capacity = max(2, 2 * nblk // writers)
    f32 = jnp.float32

    vw, uw, uv = velocity[1:], velocity[::2], velocity[:2]
    xb, xa = faces((vw[:, 0], vw[:, -1]), "gx")
    yb, ya = faces((uw[:, :, 0], uw[:, :, -1]), "gy")

    def z_face(f):
        return jnp.pad(f.transpose(0, 2, 1), ((0, 0), (0, 0), (0, cells_z - cells_x)))

    zb, za = faces((z_face(uv[..., 0]), z_face(uv[..., -1])), "wa")

    slots = pl.pallas_call(
        functools.partial(slot_kernel, writers, capacity),
        out_shape=jax.ShapeDtypeStruct((nblk // 128, 128), jnp.int32),
        name="slots",
    )(destinations.reshape(nblk // 128, 128))

    table = jnp.asarray(split_table())
    smem = pl.BlockSpec(memory_space=pltpu.SMEM)
    vmem = pl.BlockSpec(memory_space=pltpu.VMEM)
    outgoing, squares = pl.pallas_call(
        blocks_kernel,
        out_shape=(
            jax.ShapeDtypeStruct((comps * writers * capacity, width), f32),
            jax.ShapeDtypeStruct((8, cells_z), f32),
        ),
        in_specs=[smem, smem] + [vmem] * 8,
        out_specs=(vmem, vmem),
        scratch_shapes=[pltpu.VMEM((comps, nblk, width), f32)],
        compiler_params=pltpu.CompilerParams(vmem_limit_bytes=48 * 2**20),
        name="blocks",
    )(slots.reshape(nblk), lengths.reshape(nblk), velocity, xb, xa, yb, ya, zb, za, table)
    outgoing = outgoing.reshape(comps, writers, capacity, width)

    anywhere = pl.BlockSpec(memory_space=pl.ANY)
    arrived = pl.pallas_call(
        functools.partial(exchange_kernel, n_x, n_y),
        out_shape=jax.ShapeDtypeStruct(outgoing.shape, f32),
        in_specs=[anywhere],
        out_specs=anywhere,
        scratch_shapes=[
            pltpu.SemaphoreType.DMA((writers - 1,)),
            pltpu.SemaphoreType.DMA((writers - 1,)),
        ],
        compiler_params=pltpu.CompilerParams(collective_id=0, has_side_effects=True),
        name="exchange",
    )(outgoing)

    squares = lax.psum(squares, ("gx", "gy", "wa"))
    every = velocity.size * n_x * n_y * n_z
    me = (lax.axis_index("gx") * n_y + lax.axis_index("gy")).astype(jnp.int32).reshape(1)
    block = (1, 1, capacity, width)
    received = pl.pallas_call(
        functools.partial(scale_kernel, float(every)),
        grid_spec=pltpu.PrefetchScalarGridSpec(
            num_scalar_prefetch=1,
            grid=(comps, writers),
            in_specs=[
                pl.BlockSpec((8, cells_z), lambda i, s, me: (0, 0)),
                pl.BlockSpec(block, lambda i, s, me: (i, s, 0, 0)),
                pl.BlockSpec(block, lambda i, s, me: (i, me[0], 0, 0)),
            ],
            out_specs=pl.BlockSpec(block, lambda i, s, me: (i, s, 0, 0)),
        ),
        out_shape=jax.ShapeDtypeStruct(outgoing.shape, f32),
        name="scale",
    )(me, squares, arrived, outgoing)
    return received.reshape(1, 1, comps, writers, capacity, width)


def solution(mesh):
    return jax.shard_map(
        local,
        mesh=mesh,
        in_specs=(
            P(None, "gx", "gy", "wa"),
            P("gx", "gy", "wa", None),
            P("gx", "gy", "wa", None, None),
        ),
        out_specs=P(("gx", "gy"), "wa", None, None, None, None),
        check_vma=False,
    )
```

```python
import functools

import jax
import jax.numpy as jnp
import numpy as np
from jax import lax
from jax.experimental import pallas as pl
from jax.experimental.pallas import tpu as pltpu
from jax.sharding import PartitionSpec as P

BY = 8
BZ = 16
MESH = pl.DeviceIdType.MESH


def dct_table(count):
    freqs, points = np.arange(count)[:, None], np.arange(count)[None, :]
    table = np.cos(np.pi * (points + 0.5) * freqs / count) * np.sqrt(2.0 / count)
    return np.where(freqs == 0, table * np.sqrt(0.5), table)


def split_table():
    kron = np.kron(dct_table(BY), dct_table(BZ)).T.astype(np.float32)
    high = kron.astype(jnp.bfloat16)
    low = (kron - high.astype(np.float32)).astype(jnp.bfloat16)
    return np.block([[high, low], [high, np.zeros_like(low)]]).astype(jnp.bfloat16)


def faces(array, axis):
    peers = lax.axis_size(axis)
    up = [(i, (i + 1) % peers) for i in range(peers)]
    down = [(j, i) for i, j in up]
    first, last = array
    return lax.ppermute(last, axis, up), lax.ppermute(first, axis, down)


def slot_kernel(writers, capacity, targets, slots):
    t = targets[...]
    rows, lanes = t.shape
    shape = (lanes, lanes)
    upper = (
        lax.broadcasted_iota(jnp.int32, shape, 0) < lax.broadcasted_iota(jnp.int32, shape, 1)
    ).astype(jnp.float32).astype(jnp.bfloat16)
    square = (rows, rows)
    lower = (
        lax.broadcasted_iota(jnp.int32, square, 1) < lax.broadcasted_iota(jnp.int32, square, 0)
    ).astype(jnp.float32).astype(jnp.bfloat16)

    def body(w, acc):
        mine = t == w
        ones = mine.astype(jnp.float32).astype(jnp.bfloat16)
        inner = jnp.dot(ones, upper, preferred_element_type=jnp.float32)
        before = jnp.dot(lower, ones, preferred_element_type=jnp.float32)
        rank = inner + jnp.sum(before, axis=1, keepdims=True)
        return jnp.where(mine, w * capacity + rank.astype(jnp.int32), acc)

    slots[...] = lax.fori_loop(0, writers, body, jnp.zeros_like(t))


def block_rows(plane):
    cells_y, cells_z = plane.shape
    tiles = plane.reshape(cells_y // BY, BY, cells_z)
    sub = lax.broadcasted_iota(jnp.int32, tiles.shape, 1)
    group = lax.broadcasted_iota(jnp.int32, tiles.shape, 2) // BZ
    k = 1
    while k < BY:
        s_bit, g_bit = (sub & k) != 0, (group & k) != 0
        fwd = pltpu.roll(pltpu.roll(tiles, BY - k, 1), k * BZ, 2)
        back = pltpu.roll(pltpu.roll(tiles, k, 1), cells_z - k * BZ, 2)
        tiles = jnp.where(s_bit == g_bit, tiles, jnp.where(g_bit, fwd, back))
        k *= 2
    return tiles.reshape(cells_y, cells_z)


def blocks_kernel(
    slots, lens, vel, xb, xa, yb, ya, zb, za, table, out, squares, coeffs
):
    comps, cells_x, cells_y, cells_z = vel.shape
    nblk = coeffs.shape[1]
    per_plane = nblk // cells_x
    rows = out.shape[0] // comps
    width = out.shape[1]
    row = lax.broadcasted_iota(jnp.int32, (cells_y, cells_z), 0)
    lane = lax.broadcasted_iota(jnp.int32, (cells_y, cells_z), 1)
    chunk = 128

    def clear(i, _):
        out[pl.ds(pl.multiple_of(i * chunk, chunk), chunk), :] = jnp.zeros(
            (chunk, width), jnp.float32
        )
        return 0

    lax.fori_loop(0, out.shape[0] // chunk, clear, 0)

    def plane(x, acc):
        u, v, w = vel[0, x], vel[1, x], vel[2, x]

        def along_x(comp):
            nxt = jnp.where(
                x == cells_x - 1, xa[comp - 1], vel[comp, jnp.minimum(x + 1, cells_x - 1)]
            )
            prv = jnp.where(x == 0, xb[comp - 1], vel[comp, jnp.maximum(x - 1, 0)])
            return (nxt - prv) * 0.5

        def along_y(f, face):
            nxt = jnp.where(
                row == cells_y - 1, ya[face, pl.ds(x, 1), :], pltpu.roll(f, cells_y - 1, 0)
            )
            prv = jnp.where(row == 0, yb[face, pl.ds(x, 1), :], pltpu.roll(f, 1, 0))
            return (nxt - prv) * 0.5

        def along_z(f, face):
            after = pltpu.roll(za[face], cells_z - 1 - x, 1)
            before = pltpu.roll(zb[face], lax.rem(cells_z - x, cells_z), 1)
            nxt = jnp.where(lane == cells_z - 1, after, pltpu.roll(f, cells_z - 1, 1))
            prv = jnp.where(lane == 0, before, pltpu.roll(f, 1, 1))
            return (nxt - prv) * 0.5

        curl = (
            along_y(w, 1) - along_z(v, 1),
            along_z(u, 0) - along_x(2),
            along_x(1) - along_y(u, 0),
        )
        for c in curl:
            acc = acc + jnp.sum((c * c).reshape(cells_y // 8, 8, cells_z), axis=0)
        flat = jnp.concatenate([block_rows(c) for c in curl], axis=0)
        high = flat.astype(jnp.bfloat16)
        low = (flat - high.astype(jnp.float32)).astype(jnp.bfloat16)
        both = jnp.dot(
            jnp.concatenate([high, low], axis=1), table[...], preferred_element_type=jnp.float32
        )
        result = both[:, :width] + both[:, width:]
        start = pl.multiple_of(x * per_plane, 8)
        for c in range(comps):
            coeffs[c, pl.ds(start, per_plane), :] = result[c * per_plane : (c + 1) * per_plane]
        return acc

    squares[...] = lax.fori_loop(0, cells_x, plane, jnp.zeros((8, cells_z), jnp.float32))
    freqs = lax.broadcasted_iota(jnp.int32, (1, width), 1)
    group = 8

    def place(j, _):
        for k in range(group):
            i = j * group + k
            slot, keep = slots[i], freqs < lens[i]
            for c in range(comps):
                out[pl.ds(c * rows + slot, 1), :] = jnp.where(
                    keep, coeffs[c, pl.ds(i, 1), :], 0.0
                )
        return 0

    lax.fori_loop(0, nblk // group, place, 0)


def exchange_kernel(
    n_x, n_y, n_z, send, squares, recv, total, near, far, send_sem, recv_sem, part_send, part_recv,
    own_sem,
):
    a, b = lax.axis_index("gx"), lax.axis_index("gy")
    c = lax.axis_index("wa")
    me = a * n_y + b
    offsets = [(i, j) for i in range(n_x) for j in range(n_y) if i or j]
    offsets.sort(key=lambda o: (bool(o[0]) and bool(o[1]), min(o[1], n_y - o[1])))
    peers = [(lax.rem(a + i, n_x), lax.rem(b + j, n_y), c) for i, j in offsets]
    mates = [(a, b, lax.rem(c + k, n_z)) for k in range(1, n_z)]
    barrier = pltpu.get_barrier_semaphore()
    for device in mates + peers:
        pl.semaphore_signal(barrier, inc=1, device_id=device, device_id_type=MESH)
    pl.semaphore_wait(barrier, len(peers) + len(mates))

    def start(src, dst, sems, device):
        copy = pltpu.make_async_remote_copy(
            src_ref=src,
            dst_ref=dst,
            send_sem=sems[0],
            recv_sem=sems[1],
            device_id=device,
            device_id_type=MESH,
        )
        copy.start()
        return copy

    own = pltpu.make_async_copy(squares, near.at[c], own_sem)
    own.start()
    first = [
        start(squares, near.at[c], (part_send.at[k], part_recv.at[k]), device)
        for k, device in enumerate(mates)
    ]
    copies = [
        start(
            send.at[:, device[0] * n_y + device[1]],
            recv.at[:, me],
            (send_sem.at[k], recv_sem.at[k]),
            device,
        )
        for k, device in enumerate(peers)
    ]
    own.wait()
    for copy in first:
        copy.wait()
    for k, device in enumerate(peers):
        sem = n_z - 1 + k
        copies.append(start(near, far.at[k], (part_send.at[sem], part_recv.at[sem]), device))
    for copy in copies:
        copy.wait()
    total[...] = jnp.sum(near[...], axis=0) + jnp.sum(far[...], axis=(0, 1))


def scale_kernel(every, me, squares, recv, send, out):
    total = jnp.sum(squares[...], keepdims=True)
    scale = 1.0 / jnp.sqrt(total / every + 1e-06)
    own = pl.program_id(0) == me[0]

    @pl.when(own)
    def _():
        out[...] = send[...] * scale[None, None]

    @pl.when(jnp.logical_not(own))
    def _():
        out[...] = recv[...] * scale[None, None]


def local(velocity, lengths, destinations):
    n_x, n_y, n_z = lax.axis_size("gx"), lax.axis_size("gy"), lax.axis_size("wa")
    comps, cells_x, cells_y, cells_z = velocity.shape
    width = BY * BZ
    nblk = cells_x * cells_y * cells_z // width
    writers = n_x * n_y
    capacity = max(2, 2 * nblk // writers)
    f32 = jnp.float32

    vw, uw, uv = velocity[1:], velocity[::2], velocity[:2]
    xb, xa = faces((vw[:, 0], vw[:, -1]), "gx")
    yb, ya = faces((uw[:, :, 0], uw[:, :, -1]), "gy")

    def z_face(f):
        return jnp.pad(f.transpose(0, 2, 1), ((0, 0), (0, 0), (0, cells_z - cells_x)))

    zb, za = faces((z_face(uv[..., 0]), z_face(uv[..., -1])), "wa")

    slots = pl.pallas_call(
        functools.partial(slot_kernel, writers, capacity),
        out_shape=jax.ShapeDtypeStruct((nblk // 128, 128), jnp.int32),
        name="slots",
    )(destinations.reshape(nblk // 128, 128))

    table = jnp.asarray(split_table())
    smem = pl.BlockSpec(memory_space=pltpu.SMEM)
    vmem = pl.BlockSpec(memory_space=pltpu.VMEM)
    outgoing, squares = pl.pallas_call(
        blocks_kernel,
        out_shape=(
            jax.ShapeDtypeStruct((comps * writers * capacity, width), f32),
            jax.ShapeDtypeStruct((8, cells_z), f32),
        ),
        in_specs=[smem, smem] + [vmem] * 8,
        out_specs=(vmem, vmem),
        scratch_shapes=[pltpu.VMEM((comps, nblk, width), f32)],
        compiler_params=pltpu.CompilerParams(vmem_limit_bytes=48 * 2**20),
        name="blocks",
    )(slots.reshape(nblk), lengths.reshape(nblk), velocity, xb, xa, yb, ya, zb, za, table)
    outgoing = outgoing.reshape(comps, writers, capacity, width)

    anywhere = pl.BlockSpec(memory_space=pl.ANY)
    arrived, squares = pl.pallas_call(
        functools.partial(exchange_kernel, n_x, n_y, n_z),
        out_shape=(
            jax.ShapeDtypeStruct(outgoing.shape, f32),
            jax.ShapeDtypeStruct(squares.shape, f32),
        ),
        in_specs=[anywhere, vmem],
        out_specs=(anywhere, vmem),
        scratch_shapes=[
            pltpu.VMEM((n_z,) + squares.shape, f32),
            pltpu.VMEM((writers - 1, n_z) + squares.shape, f32),
            pltpu.SemaphoreType.DMA((writers - 1,)),
            pltpu.SemaphoreType.DMA((writers - 1,)),
            pltpu.SemaphoreType.DMA((writers + n_z - 2,)),
            pltpu.SemaphoreType.DMA((writers + n_z - 2,)),
            pltpu.SemaphoreType.DMA,
        ],
        compiler_params=pltpu.CompilerParams(collective_id=0, has_side_effects=True),
        name="exchange",
    )(outgoing, squares)

    every = velocity.size * n_x * n_y * n_z
    me = (lax.axis_index("gx") * n_y + lax.axis_index("gy")).astype(jnp.int32).reshape(1)
    block = (comps, 1, capacity, width)
    received = pl.pallas_call(
        functools.partial(scale_kernel, float(every)),
        grid_spec=pltpu.PrefetchScalarGridSpec(
            num_scalar_prefetch=1,
            grid=(writers,),
            in_specs=[
                pl.BlockSpec((8, cells_z), lambda s, me: (0, 0)),
                pl.BlockSpec(block, lambda s, me: (0, s, 0, 0)),
                pl.BlockSpec(block, lambda s, me: (0, me[0], 0, 0)),
            ],
            out_specs=pl.BlockSpec(block, lambda s, me: (0, s, 0, 0)),
        ),
        out_shape=jax.ShapeDtypeStruct(outgoing.shape, f32),
        name="scale",
    )(me, squares, arrived, outgoing)
    return received.reshape(1, 1, comps, writers, capacity, width)


def solution(mesh):
    return jax.shard_map(
        local,
        mesh=mesh,
        in_specs=(
            P(None, "gx", "gy", "wa"),
            P("gx", "gy", "wa", None),
            P("gx", "gy", "wa", None, None),
        ),
        out_specs=P(("gx", "gy"), "wa", None, None, None, None),
        check_vma=False,
    )
```

```python
import functools

import jax
import jax.numpy as jnp
import numpy as np
from jax import lax
from jax.experimental import pallas as pl
from jax.experimental.pallas import tpu as pltpu
from jax.sharding import PartitionSpec as P

BY = 8
BZ = 16
MESH = pl.DeviceIdType.MESH


def dct_table(count):
    freqs, points = np.arange(count)[:, None], np.arange(count)[None, :]
    table = np.cos(np.pi * (points + 0.5) * freqs / count) * np.sqrt(2.0 / count)
    return np.where(freqs == 0, table * np.sqrt(0.5), table)


def split_table():
    kron = np.kron(dct_table(BY), dct_table(BZ)).T.astype(np.float32)
    high = kron.astype(jnp.bfloat16)
    low = (kron - high.astype(np.float32)).astype(jnp.bfloat16)
    return np.block([[high, low], [high, np.zeros_like(low)]]).astype(jnp.bfloat16)


def faces_kernel(writers, capacity, targets, vel, slots, y_faces, z_faces):
    comps, cells_x, cells_y, cells_z = vel.shape
    lane = lax.broadcasted_iota(jnp.int32, (cells_y, cells_z), 1)

    def plane(x, acc):
        here = lane == x
        rolled = [
            pltpu.roll(vel[comp, x], lax.rem(x + last, cells_z), 1)
            for last in range(2)
            for comp in (0, 1)
        ]
        for i, comp in enumerate((0, 2)):
            y_faces[0, i, pl.ds(x, 1), :] = vel[comp, x, 0:1]
            y_faces[1, i, pl.ds(x, 1), :] = vel[comp, x, cells_y - 1 : cells_y]
        return tuple(jnp.where(here, new, old) for new, old in zip(rolled, acc))

    zero = jnp.zeros((cells_y, cells_z), jnp.float32)
    columns = lax.fori_loop(0, cells_x, plane, (zero,) * 4)
    for last in range(2):
        for i in range(2):
            z_faces[last, i] = columns[2 * last + i]

    t = targets[...]
    rows, lanes = t.shape
    shape = (lanes, lanes)
    upper = (
        lax.broadcasted_iota(jnp.int32, shape, 0) < lax.broadcasted_iota(jnp.int32, shape, 1)
    ).astype(jnp.float32).astype(jnp.bfloat16)
    square = (rows, rows)
    lower = (
        lax.broadcasted_iota(jnp.int32, square, 1) < lax.broadcasted_iota(jnp.int32, square, 0)
    ).astype(jnp.float32).astype(jnp.bfloat16)

    def body(w, acc):
        mine = t == w
        ones = mine.astype(jnp.float32).astype(jnp.bfloat16)
        inner = jnp.dot(ones, upper, preferred_element_type=jnp.float32)
        before = jnp.dot(lower, ones, preferred_element_type=jnp.float32)
        rank = inner + jnp.sum(before, axis=1, keepdims=True)
        return jnp.where(mine, w * capacity + rank.astype(jnp.int32), acc)

    slots[...] = lax.fori_loop(0, writers, body, jnp.zeros_like(t))


def halo_kernel(sizes, vel, y_faces, z_faces, xb, xa, yb, ya, zb, za, send_sem, recv_sem):
    place = [lax.axis_index(axis) for axis in ("gx", "gy", "wa")]
    cells_x = vel.shape[1]

    def beside(axis, step):
        size = sizes[axis]
        moved = lax.rem(place[axis] + step + size, size)
        return tuple(moved if i == axis else p for i, p in enumerate(place))

    moves = [
        (vel.at[pl.ds(1, 2), cells_x - 1], xb, beside(0, 1)),
        (vel.at[pl.ds(1, 2), 0], xa, beside(0, -1)),
        (y_faces.at[1], yb, beside(1, 1)),
        (y_faces.at[0], ya, beside(1, -1)),
        (z_faces.at[1], zb, beside(2, 1)),
        (z_faces.at[0], za, beside(2, -1)),
    ]
    barrier = pltpu.get_barrier_semaphore()
    for _, _, device in moves:
        pl.semaphore_signal(barrier, inc=1, device_id=device, device_id_type=MESH)
    pl.semaphore_wait(barrier, len(moves))
    copies = []
    for k, (src, dst, device) in enumerate(moves):
        copy = pltpu.make_async_remote_copy(
            src_ref=src,
            dst_ref=dst,
            send_sem=send_sem.at[k],
            recv_sem=recv_sem.at[k],
            device_id=device,
            device_id_type=MESH,
        )
        copy.start()
        copies.append(copy)
    for copy in copies:
        copy.wait()


def block_rows(plane):
    cells_y, cells_z = plane.shape
    tiles = plane.reshape(cells_y // BY, BY, cells_z)
    sub = lax.broadcasted_iota(jnp.int32, tiles.shape, 1)
    group = lax.broadcasted_iota(jnp.int32, tiles.shape, 2) // BZ
    k = 1
    while k < BY:
        s_bit, g_bit = (sub & k) != 0, (group & k) != 0
        fwd = pltpu.roll(pltpu.roll(tiles, BY - k, 1), k * BZ, 2)
        back = pltpu.roll(pltpu.roll(tiles, k, 1), cells_z - k * BZ, 2)
        tiles = jnp.where(s_bit == g_bit, tiles, jnp.where(g_bit, fwd, back))
        k *= 2
    return tiles.reshape(cells_y, cells_z)


def blocks_kernel(
    slots, lens, vel, xb, xa, yb, ya, zb, za, table, out, squares, coeffs
):
    comps, cells_x, cells_y, cells_z = vel.shape
    nblk = coeffs.shape[1]
    per_plane = nblk // cells_x
    rows = out.shape[0] // comps
    width = out.shape[1]
    row = lax.broadcasted_iota(jnp.int32, (cells_y, cells_z), 0)
    lane = lax.broadcasted_iota(jnp.int32, (cells_y, cells_z), 1)
    chunk = 128

    def clear(i, _):
        out[pl.ds(pl.multiple_of(i * chunk, chunk), chunk), :] = jnp.zeros(
            (chunk, width), jnp.float32
        )
        return 0

    lax.fori_loop(0, out.shape[0] // chunk, clear, 0)

    def plane(x, acc):
        u, v, w = vel[0, x], vel[1, x], vel[2, x]

        def along_x(comp):
            nxt = jnp.where(
                x == cells_x - 1, xa[comp - 1], vel[comp, jnp.minimum(x + 1, cells_x - 1)]
            )
            prv = jnp.where(x == 0, xb[comp - 1], vel[comp, jnp.maximum(x - 1, 0)])
            return (nxt - prv) * 0.5

        def along_y(f, face):
            nxt = jnp.where(
                row == cells_y - 1, ya[face, pl.ds(x, 1), :], pltpu.roll(f, cells_y - 1, 0)
            )
            prv = jnp.where(row == 0, yb[face, pl.ds(x, 1), :], pltpu.roll(f, 1, 0))
            return (nxt - prv) * 0.5

        def along_z(f, face):
            after = pltpu.roll(za[face], cells_z - 1 - x, 1)
            before = pltpu.roll(zb[face], lax.rem(cells_z - x, cells_z), 1)
            nxt = jnp.where(lane == cells_z - 1, after, pltpu.roll(f, cells_z - 1, 1))
            prv = jnp.where(lane == 0, before, pltpu.roll(f, 1, 1))
            return (nxt - prv) * 0.5

        curl = (
            along_y(w, 1) - along_z(v, 1),
            along_z(u, 0) - along_x(2),
            along_x(1) - along_y(u, 0),
        )
        for c in curl:
            acc = acc + jnp.sum((c * c).reshape(cells_y // 8, 8, cells_z), axis=0)
        flat = jnp.concatenate([block_rows(c) for c in curl], axis=0)
        high = flat.astype(jnp.bfloat16)
        low = (flat - high.astype(jnp.float32)).astype(jnp.bfloat16)
        both = jnp.dot(
            jnp.concatenate([high, low], axis=1), table[...], preferred_element_type=jnp.float32
        )
        result = both[:, :width] + both[:, width:]
        start = pl.multiple_of(x * per_plane, 8)
        for c in range(comps):
            coeffs[c, pl.ds(start, per_plane), :] = result[c * per_plane : (c + 1) * per_plane]
        return acc

    squares[...] = lax.fori_loop(0, cells_x, plane, jnp.zeros((8, cells_z), jnp.float32))
    freqs = lax.broadcasted_iota(jnp.int32, (1, width), 1)
    group = 8

    def place(j, _):
        found = []
        for k in range(group):
            i = j * group + k
            keep = freqs < lens[i]
            for c in range(comps):
                cut = jnp.where(keep, coeffs[c, pl.ds(i, 1), :], 0.0)
                found.append((c * rows + slots[i], cut))
        for spot, cut in found:
            out[pl.ds(spot, 1), :] = cut
        return 0

    lax.fori_loop(0, nblk // group, place, 0)


def exchange_kernel(
    n_x, n_y, n_z, send, squares, recv, total, near, far, send_sem, recv_sem, part_send, part_recv,
    own_sem,
):
    a, b = lax.axis_index("gx"), lax.axis_index("gy")
    c = lax.axis_index("wa")
    me = a * n_y + b
    offsets = [(i, j) for i in range(n_x) for j in range(n_y) if i or j]
    offsets.sort(key=lambda o: (bool(o[0]) and bool(o[1]), min(o[1], n_y - o[1])))
    peers = [(lax.rem(a + i, n_x), lax.rem(b + j, n_y), c) for i, j in offsets]
    mates = [(a, b, lax.rem(c + k, n_z)) for k in range(1, n_z)]
    barrier = pltpu.get_barrier_semaphore()
    for device in mates + peers:
        pl.semaphore_signal(barrier, inc=1, device_id=device, device_id_type=MESH)
    pl.semaphore_wait(barrier, len(peers) + len(mates))

    def start(src, dst, sems, device):
        copy = pltpu.make_async_remote_copy(
            src_ref=src,
            dst_ref=dst,
            send_sem=sems[0],
            recv_sem=sems[1],
            device_id=device,
            device_id_type=MESH,
        )
        copy.start()
        return copy

    own = pltpu.make_async_copy(squares, near.at[c], own_sem)
    own.start()
    first = [
        start(squares, near.at[c], (part_send.at[k], part_recv.at[k]), device)
        for k, device in enumerate(mates)
    ]
    copies = [
        start(
            send.at[:, device[0] * n_y + device[1]],
            recv.at[:, me],
            (send_sem.at[k], recv_sem.at[k]),
            device,
        )
        for k, device in enumerate(peers)
    ]
    own.wait()
    for copy in first:
        copy.wait()
    for k, device in enumerate(peers):
        sem = n_z - 1 + k
        copies.append(start(near, far.at[k], (part_send.at[sem], part_recv.at[sem]), device))
    for copy in copies:
        copy.wait()
    total[...] = jnp.sum(near[...], axis=0) + jnp.sum(far[...], axis=(0, 1))


def scale_kernel(every, me, squares, recv, send, out):
    total = jnp.sum(squares[...], keepdims=True)
    scale = 1.0 / jnp.sqrt(total / every + 1e-06)
    own = pl.program_id(0) == me[0]

    @pl.when(own)
    def _():
        out[...] = send[...] * scale[None, None]

    @pl.when(jnp.logical_not(own))
    def _():
        out[...] = recv[...] * scale[None, None]


def local(velocity, lengths, destinations):
    n_x, n_y, n_z = lax.axis_size("gx"), lax.axis_size("gy"), lax.axis_size("wa")
    comps, cells_x, cells_y, cells_z = velocity.shape
    width = BY * BZ
    nblk = cells_x * cells_y * cells_z // width
    writers = n_x * n_y
    capacity = max(2, 2 * nblk // writers)
    f32 = jnp.float32

    smem = pl.BlockSpec(memory_space=pltpu.SMEM)
    vmem = pl.BlockSpec(memory_space=pltpu.VMEM)
    anywhere = pl.BlockSpec(memory_space=pl.ANY)
    x_face = jax.ShapeDtypeStruct((2, cells_y, cells_z), f32)
    y_face = jax.ShapeDtypeStruct((2, cells_x, cells_z), f32)
    slots, y_faces, z_faces = pl.pallas_call(
        functools.partial(faces_kernel, writers, capacity),
        out_shape=(
            jax.ShapeDtypeStruct((nblk // 128, 128), jnp.int32),
            jax.ShapeDtypeStruct((2,) + y_face.shape, f32),
            jax.ShapeDtypeStruct((2,) + x_face.shape, f32),
        ),
        name="faces",
    )(destinations.reshape(nblk // 128, 128), velocity)
    halos = pl.pallas_call(
        functools.partial(halo_kernel, (n_x, n_y, n_z)),
        out_shape=(x_face, x_face, y_face, y_face, x_face, x_face),
        in_specs=[anywhere] * 3,
        out_specs=(anywhere,) * 6,
        scratch_shapes=[pltpu.SemaphoreType.DMA((6,)), pltpu.SemaphoreType.DMA((6,))],
        compiler_params=pltpu.CompilerParams(collective_id=1, has_side_effects=True),
        name="halo",
    )(velocity, y_faces, z_faces)

    table = jnp.asarray(split_table())
    outgoing, squares = pl.pallas_call(
        blocks_kernel,
        out_shape=(
            jax.ShapeDtypeStruct((comps * writers * capacity, width), f32),
            jax.ShapeDtypeStruct((8, cells_z), f32),
        ),
        in_specs=[smem, smem] + [vmem] * 8,
        out_specs=(vmem, vmem),
        scratch_shapes=[pltpu.VMEM((comps, nblk, width), f32)],
        compiler_params=pltpu.CompilerParams(vmem_limit_bytes=48 * 2**20),
        name="blocks",
    )(slots.reshape(nblk), lengths.reshape(nblk), velocity, *halos, table)
    outgoing = outgoing.reshape(comps, writers, capacity, width)

    arrived, squares = pl.pallas_call(
        functools.partial(exchange_kernel, n_x, n_y, n_z),
        out_shape=(
            jax.ShapeDtypeStruct(outgoing.shape, f32),
            jax.ShapeDtypeStruct(squares.shape, f32),
        ),
        in_specs=[anywhere, vmem],
        out_specs=(anywhere, vmem),
        scratch_shapes=[
            pltpu.VMEM((n_z,) + squares.shape, f32),
            pltpu.VMEM((writers - 1, n_z) + squares.shape, f32),
            pltpu.SemaphoreType.DMA((writers - 1,)),
            pltpu.SemaphoreType.DMA((writers - 1,)),
            pltpu.SemaphoreType.DMA((writers + n_z - 2,)),
            pltpu.SemaphoreType.DMA((writers + n_z - 2,)),
            pltpu.SemaphoreType.DMA,
        ],
        compiler_params=pltpu.CompilerParams(collective_id=0, has_side_effects=True),
        name="exchange",
    )(outgoing, squares)

    every = velocity.size * n_x * n_y * n_z
    me = (lax.axis_index("gx") * n_y + lax.axis_index("gy")).astype(jnp.int32).reshape(1)
    block = (comps, 1, capacity, width)
    received = pl.pallas_call(
        functools.partial(scale_kernel, float(every)),
        grid_spec=pltpu.PrefetchScalarGridSpec(
            num_scalar_prefetch=1,
            grid=(writers,),
            in_specs=[
                pl.BlockSpec((8, cells_z), lambda s, me: (0, 0)),
                pl.BlockSpec(block, lambda s, me: (0, s, 0, 0)),
                pl.BlockSpec(block, lambda s, me: (0, me[0], 0, 0)),
            ],
            out_specs=pl.BlockSpec(block, lambda s, me: (0, s, 0, 0)),
        ),
        out_shape=jax.ShapeDtypeStruct(outgoing.shape, f32),
        name="scale",
    )(me, squares, arrived, outgoing)
    return received.reshape(1, 1, comps, writers, capacity, width)


def solution(mesh):
    return jax.shard_map(
        local,
        mesh=mesh,
        in_specs=(
            P(None, "gx", "gy", "wa"),
            P("gx", "gy", "wa", None),
            P("gx", "gy", "wa", None, None),
        ),
        out_specs=P(("gx", "gy"), "wa", None, None, None, None),
        check_vma=False,
    )
```

```python
import functools

import jax
import jax.numpy as jnp
import numpy as np
from jax import lax
from jax.experimental import pallas as pl
from jax.experimental.pallas import tpu as pltpu
from jax.sharding import PartitionSpec as P

BY = 8
BZ = 16
MESH = pl.DeviceIdType.MESH


def dct_table(count):
    freqs, points = np.arange(count)[:, None], np.arange(count)[None, :]
    table = np.cos(np.pi * (points + 0.5) * freqs / count) * np.sqrt(2.0 / count)
    return np.where(freqs == 0, table * np.sqrt(0.5), table)


def split_table():
    kron = np.kron(dct_table(BY), dct_table(BZ)).T.astype(np.float32)
    high = kron.astype(jnp.bfloat16)
    low = (kron - high.astype(np.float32)).astype(jnp.bfloat16)
    return np.block([[high, low], [high, np.zeros_like(low)]]).astype(jnp.bfloat16)


def faces_kernel(writers, capacity, targets, vel, slots, y_faces, z_faces):
    comps, cells_x, cells_y, cells_z = vel.shape
    lane = lax.broadcasted_iota(jnp.int32, (cells_y, cells_z), 1)

    def plane(x, acc):
        here = lane == x
        rolled = [
            pltpu.roll(vel[comp, x], lax.rem(x + last, cells_z), 1)
            for last in range(2)
            for comp in (0, 1)
        ]
        for i, comp in enumerate((0, 2)):
            y_faces[0, i, pl.ds(x, 1), :] = vel[comp, x, 0:1]
            y_faces[1, i, pl.ds(x, 1), :] = vel[comp, x, cells_y - 1 : cells_y]
        return tuple(jnp.where(here, new, old) for new, old in zip(rolled, acc))

    zero = jnp.zeros((cells_y, cells_z), jnp.float32)
    columns = lax.fori_loop(0, cells_x, plane, (zero,) * 4)
    for last in range(2):
        for i in range(2):
            z_faces[last, i] = columns[2 * last + i]

    t = targets[...]
    rows, lanes = t.shape
    shape = (lanes, lanes)
    upper = (
        lax.broadcasted_iota(jnp.int32, shape, 0) < lax.broadcasted_iota(jnp.int32, shape, 1)
    ).astype(jnp.float32).astype(jnp.bfloat16)
    square = (rows, rows)
    lower = (
        lax.broadcasted_iota(jnp.int32, square, 1) < lax.broadcasted_iota(jnp.int32, square, 0)
    ).astype(jnp.float32).astype(jnp.bfloat16)

    def body(w, acc):
        mine = t == w
        ones = mine.astype(jnp.float32).astype(jnp.bfloat16)
        inner = jnp.dot(ones, upper, preferred_element_type=jnp.float32)
        before = jnp.dot(lower, ones, preferred_element_type=jnp.float32)
        rank = inner + jnp.sum(before, axis=1, keepdims=True)
        return jnp.where(mine, w * capacity + rank.astype(jnp.int32), acc)

    slots[...] = lax.fori_loop(0, writers, body, jnp.zeros_like(t))


def halo_kernel(sizes, vel, y_faces, z_faces, halos, send_sem, recv_sem):
    place = [lax.axis_index(axis) for axis in ("gx", "gy", "wa")]
    cells_x = vel.shape[1]

    def beside(axis, step):
        size = sizes[axis]
        moved = lax.rem(place[axis] + step + size, size)
        return tuple(moved if i == axis else p for i, p in enumerate(place))

    across, along = pl.ds(0, vel.shape[2]), pl.ds(0, cells_x)
    moves = [
        (vel.at[pl.ds(1, 2), cells_x - 1], halos.at[0, :, across], beside(0, 1)),
        (vel.at[pl.ds(1, 2), 0], halos.at[1, :, across], beside(0, -1)),
        (y_faces.at[1], halos.at[2, :, along], beside(1, 1)),
        (y_faces.at[0], halos.at[3, :, along], beside(1, -1)),
        (z_faces.at[1], halos.at[4, :, across], beside(2, 1)),
        (z_faces.at[0], halos.at[5, :, across], beside(2, -1)),
    ]
    barrier = pltpu.get_barrier_semaphore()
    for _, _, device in moves:
        pl.semaphore_signal(barrier, inc=1, device_id=device, device_id_type=MESH)
    pl.semaphore_wait(barrier, len(moves))
    copies = []
    for k, (src, dst, device) in enumerate(moves):
        copy = pltpu.make_async_remote_copy(
            src_ref=src,
            dst_ref=dst,
            send_sem=send_sem.at[k],
            recv_sem=recv_sem.at[k],
            device_id=device,
            device_id_type=MESH,
        )
        copy.start()
        copies.append(copy)
    for copy in copies:
        copy.wait()


def block_rows(plane):
    cells_y, cells_z = plane.shape
    tiles = plane.reshape(cells_y // BY, BY, cells_z)
    sub = lax.broadcasted_iota(jnp.int32, tiles.shape, 1)
    group = lax.broadcasted_iota(jnp.int32, tiles.shape, 2) // BZ
    k = 1
    while k < BY:
        s_bit, g_bit = (sub & k) != 0, (group & k) != 0
        fwd = pltpu.roll(pltpu.roll(tiles, BY - k, 1), k * BZ, 2)
        back = pltpu.roll(pltpu.roll(tiles, k, 1), cells_z - k * BZ, 2)
        tiles = jnp.where(s_bit == g_bit, tiles, jnp.where(g_bit, fwd, back))
        k *= 2
    return tiles.reshape(cells_y, cells_z)


def blocks_kernel(slots, lens, vel, halos, table, out, squares, coeffs):
    comps, cells_x, cells_y, cells_z = vel.shape
    nblk = coeffs.shape[1]
    per_plane = nblk // cells_x
    rows = out.shape[0] // comps
    width = out.shape[1]
    row = lax.broadcasted_iota(jnp.int32, (cells_y, cells_z), 0)
    lane = lax.broadcasted_iota(jnp.int32, (cells_y, cells_z), 1)
    chunk = 128

    def clear(i, _):
        out[pl.ds(pl.multiple_of(i * chunk, chunk), chunk), :] = jnp.zeros(
            (chunk, width), jnp.float32
        )
        return 0

    lax.fori_loop(0, out.shape[0] // chunk, clear, 0)

    def plane(x, acc):
        u, v, w = vel[0, x], vel[1, x], vel[2, x]

        def along_x(comp):
            nxt = jnp.where(
                x == cells_x - 1, halos[1, comp - 1, :cells_y], vel[comp, jnp.minimum(x + 1, cells_x - 1)]
            )
            prv = jnp.where(x == 0, halos[0, comp - 1, :cells_y], vel[comp, jnp.maximum(x - 1, 0)])
            return (nxt - prv) * 0.5

        def along_y(f, face):
            nxt = jnp.where(
                row == cells_y - 1, halos[3, face, pl.ds(x, 1), :], pltpu.roll(f, cells_y - 1, 0)
            )
            prv = jnp.where(row == 0, halos[2, face, pl.ds(x, 1), :], pltpu.roll(f, 1, 0))
            return (nxt - prv) * 0.5

        def along_z(f, face):
            after = pltpu.roll(halos[5, face, :cells_y], cells_z - 1 - x, 1)
            before = pltpu.roll(halos[4, face, :cells_y], lax.rem(cells_z - x, cells_z), 1)
            nxt = jnp.where(lane == cells_z - 1, after, pltpu.roll(f, cells_z - 1, 1))
            prv = jnp.where(lane == 0, before, pltpu.roll(f, 1, 1))
            return (nxt - prv) * 0.5

        curl = (
            along_y(w, 1) - along_z(v, 1),
            along_z(u, 0) - along_x(2),
            along_x(1) - along_y(u, 0),
        )
        for c in curl:
            acc = acc + jnp.sum((c * c).reshape(cells_y // 8, 8, cells_z), axis=0)
        flat = jnp.concatenate([block_rows(c) for c in curl], axis=0)
        high = flat.astype(jnp.bfloat16)
        low = (flat - high.astype(jnp.float32)).astype(jnp.bfloat16)
        both = jnp.dot(
            jnp.concatenate([high, low], axis=1), table[...], preferred_element_type=jnp.float32
        )
        result = both[:, :width] + both[:, width:]
        start = pl.multiple_of(x * per_plane, 8)
        for c in range(comps):
            coeffs[c, pl.ds(start, per_plane), :] = result[c * per_plane : (c + 1) * per_plane]
        return acc

    freqs = lax.broadcasted_iota(jnp.int32, (1, width), 1)
    group = 8

    def place(x):
        for start in range(0, per_plane, group):
            found = []
            for k in range(start, min(start + group, per_plane)):
                i = x * per_plane + k
                keep = freqs < lens[i]
                for c in range(comps):
                    cut = jnp.where(keep, coeffs[c, pl.ds(i, 1), :], 0.0)
                    found.append((c * rows + slots[i], cut))
            for spot, cut in found:
                out[pl.ds(spot, 1), :] = cut

    def step(x, acc):
        place(x - 1)
        return plane(x, acc)

    first = plane(0, jnp.zeros((8, cells_z), jnp.float32))
    squares[...] = lax.fori_loop(1, cells_x, step, first)
    place(cells_x - 1)


def exchange_kernel(
    n_x, n_y, n_z, send, squares, recv, total, near, far, send_sem, recv_sem, part_send, part_recv,
    own_sem,
):
    a, b = lax.axis_index("gx"), lax.axis_index("gy")
    c = lax.axis_index("wa")
    me = a * n_y + b
    offsets = [(i, j) for i in range(n_x) for j in range(n_y) if i or j]
    offsets.sort(key=lambda o: (bool(o[0]) and bool(o[1]), min(o[1], n_y - o[1])))
    peers = [(lax.rem(a + i, n_x), lax.rem(b + j, n_y), c) for i, j in offsets]
    mates = [(a, b, lax.rem(c + k, n_z)) for k in range(1, n_z)]
    barrier = pltpu.get_barrier_semaphore()
    for device in mates + peers:
        pl.semaphore_signal(barrier, inc=1, device_id=device, device_id_type=MESH)
    pl.semaphore_wait(barrier, len(peers) + len(mates))

    def start(src, dst, sems, device):
        copy = pltpu.make_async_remote_copy(
            src_ref=src,
            dst_ref=dst,
            send_sem=sems[0],
            recv_sem=sems[1],
            device_id=device,
            device_id_type=MESH,
        )
        copy.start()
        return copy

    own = pltpu.make_async_copy(squares, near.at[c], own_sem)
    own.start()
    first = [
        start(squares, near.at[c], (part_send.at[k], part_recv.at[k]), device)
        for k, device in enumerate(mates)
    ]
    def blocks_to(k):
        device = peers[k]
        return start(
            send.at[:, device[0] * n_y + device[1]],
            recv.at[:, me],
            (send_sem.at[k], recv_sem.at[k]),
            device,
        )

    ahead = min(3, len(peers))
    copies = [blocks_to(k) for k in range(ahead)]
    own.wait()
    for copy in first:
        copy.wait()
    for k, device in enumerate(peers):
        sem = n_z - 1 + k
        copies.append(start(near, far.at[k], (part_send.at[sem], part_recv.at[sem]), device))
    copies += [blocks_to(k) for k in range(ahead, len(peers))]
    for copy in copies:
        copy.wait()
    total[...] = jnp.sum(near[...], axis=0) + jnp.sum(far[...], axis=(0, 1))


def scale_kernel(every, me, squares, recv, send, out):
    total = jnp.sum(squares[...], keepdims=True)
    scale = 1.0 / jnp.sqrt(total / every + 1e-06)
    own = pl.program_id(0) == me[0]

    @pl.when(own)
    def _():
        out[...] = send[...] * scale[None, None]

    @pl.when(jnp.logical_not(own))
    def _():
        out[...] = recv[...] * scale[None, None]


def local(velocity, lengths, destinations):
    n_x, n_y, n_z = lax.axis_size("gx"), lax.axis_size("gy"), lax.axis_size("wa")
    comps, cells_x, cells_y, cells_z = velocity.shape
    width = BY * BZ
    nblk = cells_x * cells_y * cells_z // width
    writers = n_x * n_y
    capacity = max(2, 2 * nblk // writers)
    f32 = jnp.float32

    smem = pl.BlockSpec(memory_space=pltpu.SMEM)
    vmem = pl.BlockSpec(memory_space=pltpu.VMEM)
    anywhere = pl.BlockSpec(memory_space=pl.ANY)
    slots, y_faces, z_faces = pl.pallas_call(
        functools.partial(faces_kernel, writers, capacity),
        out_shape=(
            jax.ShapeDtypeStruct((nblk // 128, 128), jnp.int32),
            jax.ShapeDtypeStruct((2, 2, cells_x, cells_z), f32),
            jax.ShapeDtypeStruct((2, 2, cells_y, cells_z), f32),
        ),
        name="faces",
    )(destinations.reshape(nblk // 128, 128), velocity)
    halos = pl.pallas_call(
        functools.partial(halo_kernel, (n_x, n_y, n_z)),
        out_shape=jax.ShapeDtypeStruct((6, 2, max(cells_x, cells_y), cells_z), f32),
        in_specs=[anywhere] * 3,
        out_specs=anywhere,
        scratch_shapes=[pltpu.SemaphoreType.DMA((6,)), pltpu.SemaphoreType.DMA((6,))],
        compiler_params=pltpu.CompilerParams(collective_id=1, has_side_effects=True),
        name="halo",
    )(velocity, y_faces, z_faces)

    table = jnp.asarray(split_table())
    outgoing, squares = pl.pallas_call(
        blocks_kernel,
        out_shape=(
            jax.ShapeDtypeStruct((comps * writers * capacity, width), f32),
            jax.ShapeDtypeStruct((8, cells_z), f32),
        ),
        in_specs=[smem, smem] + [vmem] * 3,
        out_specs=(vmem, vmem),
        scratch_shapes=[pltpu.VMEM((comps, nblk, width), f32)],
        compiler_params=pltpu.CompilerParams(vmem_limit_bytes=48 * 2**20),
        name="blocks",
    )(slots.reshape(nblk), lengths.reshape(nblk), velocity, halos, table)
    outgoing = outgoing.reshape(comps, writers, capacity, width)

    arrived, squares = pl.pallas_call(
        functools.partial(exchange_kernel, n_x, n_y, n_z),
        out_shape=(
            jax.ShapeDtypeStruct(outgoing.shape, f32),
            jax.ShapeDtypeStruct(squares.shape, f32),
        ),
        in_specs=[anywhere, vmem],
        out_specs=(anywhere, vmem),
        scratch_shapes=[
            pltpu.VMEM((n_z,) + squares.shape, f32),
            pltpu.VMEM((writers - 1, n_z) + squares.shape, f32),
            pltpu.SemaphoreType.DMA((writers - 1,)),
            pltpu.SemaphoreType.DMA((writers - 1,)),
            pltpu.SemaphoreType.DMA((writers + n_z - 2,)),
            pltpu.SemaphoreType.DMA((writers + n_z - 2,)),
            pltpu.SemaphoreType.DMA,
        ],
        compiler_params=pltpu.CompilerParams(collective_id=0, has_side_effects=True),
        name="exchange",
    )(outgoing, squares)

    every = velocity.size * n_x * n_y * n_z
    me = (lax.axis_index("gx") * n_y + lax.axis_index("gy")).astype(jnp.int32).reshape(1)
    block = (comps, 1, capacity, width)
    received = pl.pallas_call(
        functools.partial(scale_kernel, float(every)),
        grid_spec=pltpu.PrefetchScalarGridSpec(
            num_scalar_prefetch=1,
            grid=(writers,),
            in_specs=[
                pl.BlockSpec((8, cells_z), lambda s, me: (0, 0)),
                pl.BlockSpec(block, lambda s, me: (0, s, 0, 0)),
                pl.BlockSpec(block, lambda s, me: (0, me[0], 0, 0)),
            ],
            out_specs=pl.BlockSpec(block, lambda s, me: (0, s, 0, 0)),
        ),
        out_shape=jax.ShapeDtypeStruct(outgoing.shape, f32),
        name="scale",
    )(me, squares, arrived, outgoing)
    return received.reshape(1, 1, comps, writers, capacity, width)


def solution(mesh):
    return jax.shard_map(
        local,
        mesh=mesh,
        in_specs=(
            P(None, "gx", "gy", "wa"),
            P("gx", "gy", "wa", None),
            P("gx", "gy", "wa", None, None),
        ),
        out_specs=P(("gx", "gy"), "wa", None, None, None, None),
        check_vma=False,
    )
```

```python
import functools

import jax
import jax.numpy as jnp
import numpy as np
from jax import lax
from jax.experimental import pallas as pl
from jax.experimental.pallas import tpu as pltpu
from jax.sharding import PartitionSpec as P

BY = 8
BZ = 16
UNROLL = 2
MESH = pl.DeviceIdType.MESH


def dct_table(count):
    freqs, points = np.arange(count)[:, None], np.arange(count)[None, :]
    table = np.cos(np.pi * (points + 0.5) * freqs / count) * np.sqrt(2.0 / count)
    return np.where(freqs == 0, table * np.sqrt(0.5), table)


def split_table():
    kron = np.kron(dct_table(BY), dct_table(BZ)).T.astype(np.float32)
    high = kron.astype(jnp.bfloat16)
    low = (kron - high.astype(np.float32)).astype(jnp.bfloat16)
    return np.block([[high, low], [high, np.zeros_like(low)]]).astype(jnp.bfloat16)


def faces_kernel(writers, capacity, targets, vel, slots, y_faces, z_faces):
    comps, cells_x, cells_y, cells_z = vel.shape
    lane = lax.broadcasted_iota(jnp.int32, (cells_y, cells_z), 1)

    def plane(x, acc):
        here = lane == x
        rolled = [
            pltpu.roll(vel[comp, x], lax.rem(x + last, cells_z), 1)
            for last in range(2)
            for comp in (0, 1)
        ]
        for i, comp in enumerate((0, 2)):
            y_faces[0, i, pl.ds(x, 1), :] = vel[comp, x, 0:1]
            y_faces[1, i, pl.ds(x, 1), :] = vel[comp, x, cells_y - 1 : cells_y]
        return tuple(jnp.where(here, new, old) for new, old in zip(rolled, acc))

    zero = jnp.zeros((cells_y, cells_z), jnp.float32)
    columns = lax.fori_loop(0, cells_x, plane, (zero,) * 4, unroll=4)
    for last in range(2):
        for i in range(2):
            z_faces[last, i] = columns[2 * last + i]

    t = targets[...]
    rows, lanes = t.shape
    shape = (lanes, lanes)
    upper = (
        lax.broadcasted_iota(jnp.int32, shape, 0) < lax.broadcasted_iota(jnp.int32, shape, 1)
    ).astype(jnp.float32).astype(jnp.bfloat16)
    square = (rows, rows)
    lower = (
        lax.broadcasted_iota(jnp.int32, square, 1) < lax.broadcasted_iota(jnp.int32, square, 0)
    ).astype(jnp.float32).astype(jnp.bfloat16)

    def body(w, acc):
        mine = t == w
        ones = mine.astype(jnp.float32).astype(jnp.bfloat16)
        inner = jnp.dot(ones, upper, preferred_element_type=jnp.float32)
        before = jnp.dot(lower, ones, preferred_element_type=jnp.float32)
        rank = inner + jnp.sum(before, axis=1, keepdims=True)
        return jnp.where(mine, w * capacity + rank.astype(jnp.int32), acc)

    slots[...] = lax.fori_loop(0, writers, body, jnp.zeros_like(t), unroll=8)


def halo_kernel(sizes, vel, y_faces, z_faces, halos, send_sem, recv_sem):
    place = [lax.axis_index(axis) for axis in ("gx", "gy", "wa")]
    cells_x = vel.shape[1]

    def beside(axis, step):
        size = sizes[axis]
        moved = lax.rem(place[axis] + step + size, size)
        return tuple(moved if i == axis else p for i, p in enumerate(place))

    across, along = pl.ds(0, vel.shape[2]), pl.ds(0, cells_x)
    moves = [
        (vel.at[pl.ds(1, 2), cells_x - 1], halos.at[0, :, across], beside(0, 1)),
        (vel.at[pl.ds(1, 2), 0], halos.at[1, :, across], beside(0, -1)),
        (y_faces.at[1], halos.at[2, :, along], beside(1, 1)),
        (y_faces.at[0], halos.at[3, :, along], beside(1, -1)),
        (z_faces.at[1], halos.at[4, :, across], beside(2, 1)),
        (z_faces.at[0], halos.at[5, :, across], beside(2, -1)),
    ]
    barrier = pltpu.get_barrier_semaphore()
    for _, _, device in moves:
        pl.semaphore_signal(barrier, inc=1, device_id=device, device_id_type=MESH)
    pl.semaphore_wait(barrier, len(moves))
    copies = []
    for k, (src, dst, device) in enumerate(moves):
        copy = pltpu.make_async_remote_copy(
            src_ref=src,
            dst_ref=dst,
            send_sem=send_sem.at[k],
            recv_sem=recv_sem.at[k],
            device_id=device,
            device_id_type=MESH,
        )
        copy.start()
        copies.append(copy)
    for copy in copies:
        copy.wait()


def block_rows(plane):
    cells_y, cells_z = plane.shape
    tiles = plane.reshape(cells_y // BY, BY, cells_z)
    sub = lax.broadcasted_iota(jnp.int32, tiles.shape, 1)
    group = lax.broadcasted_iota(jnp.int32, tiles.shape, 2) // BZ
    k = 1
    while k < BY:
        s_bit, g_bit = (sub & k) != 0, (group & k) != 0
        fwd = pltpu.roll(pltpu.roll(tiles, BY - k, 1), k * BZ, 2)
        back = pltpu.roll(pltpu.roll(tiles, k, 1), cells_z - k * BZ, 2)
        tiles = jnp.where(s_bit == g_bit, tiles, jnp.where(g_bit, fwd, back))
        k *= 2
    return tiles.reshape(cells_y, cells_z)


def blocks_kernel(slots, lens, vel, halos, table, out, squares, coeffs):
    comps, cells_x, cells_y, cells_z = vel.shape
    nblk = coeffs.shape[1]
    per_plane = nblk // cells_x
    rows = out.shape[0] // comps
    width = out.shape[1]
    row = lax.broadcasted_iota(jnp.int32, (cells_y, cells_z), 0)
    lane = lax.broadcasted_iota(jnp.int32, (cells_y, cells_z), 1)
    chunk = 128

    def clear(i, _):
        out[pl.ds(pl.multiple_of(i * chunk, chunk), chunk), :] = jnp.zeros(
            (chunk, width), jnp.float32
        )
        return 0

    lax.fori_loop(0, out.shape[0] // chunk, clear, 0)

    def plane(x, acc):
        u, v, w = vel[0, x], vel[1, x], vel[2, x]

        def along_x(comp):
            nxt = jnp.where(
                x == cells_x - 1, halos[1, comp - 1, :cells_y], vel[comp, jnp.minimum(x + 1, cells_x - 1)]
            )
            prv = jnp.where(x == 0, halos[0, comp - 1, :cells_y], vel[comp, jnp.maximum(x - 1, 0)])
            return (nxt - prv) * 0.5

        def along_y(f, face):
            nxt = jnp.where(
                row == cells_y - 1, halos[3, face, pl.ds(x, 1), :], pltpu.roll(f, cells_y - 1, 0)
            )
            prv = jnp.where(row == 0, halos[2, face, pl.ds(x, 1), :], pltpu.roll(f, 1, 0))
            return (nxt - prv) * 0.5

        def along_z(f, face):
            after = pltpu.roll(halos[5, face, :cells_y], cells_z - 1 - x, 1)
            before = pltpu.roll(halos[4, face, :cells_y], lax.rem(cells_z - x, cells_z), 1)
            nxt = jnp.where(lane == cells_z - 1, after, pltpu.roll(f, cells_z - 1, 1))
            prv = jnp.where(lane == 0, before, pltpu.roll(f, 1, 1))
            return (nxt - prv) * 0.5

        curl = (
            along_y(w, 1) - along_z(v, 1),
            along_z(u, 0) - along_x(2),
            along_x(1) - along_y(u, 0),
        )
        for c in curl:
            acc = acc + jnp.sum((c * c).reshape(cells_y // 8, 8, cells_z), axis=0)
        flat = jnp.concatenate([block_rows(c) for c in curl], axis=0)
        high = flat.astype(jnp.bfloat16)
        low = (flat - high.astype(jnp.float32)).astype(jnp.bfloat16)
        both = jnp.dot(
            jnp.concatenate([high, low], axis=1), table[...], preferred_element_type=jnp.float32
        )
        result = both[:, :width] + both[:, width:]
        start = pl.multiple_of(x * per_plane, 8)
        for c in range(comps):
            coeffs[c, pl.ds(start, per_plane), :] = result[c * per_plane : (c + 1) * per_plane]
        return acc

    freqs = lax.broadcasted_iota(jnp.int32, (1, width), 1)
    group = 8

    def place(x):
        for start in range(0, per_plane, group):
            found = []
            for k in range(start, min(start + group, per_plane)):
                i = x * per_plane + k
                keep = freqs < lens[i]
                for c in range(comps):
                    cut = jnp.where(keep, coeffs[c, pl.ds(i, 1), :], 0.0)
                    found.append((c * rows + slots[i], cut))
            for spot, cut in found:
                out[pl.ds(spot, 1), :] = cut

    together = next(n for n in (UNROLL, 2, 1) if cells_x % n == 0)

    def step(t, acc):
        for k in range(together):
            place((t - 1) * together + k)
        return planes(t, acc)

    def planes(t, acc):
        for k in range(together):
            acc = plane(t * together + k, acc)
        return acc

    first = planes(0, jnp.zeros((8, cells_z), jnp.float32))
    squares[...] = lax.fori_loop(1, cells_x // together, step, first)
    for k in range(together):
        place(cells_x - together + k)


def exchange_kernel(
    n_x, n_y, n_z, send, squares, recv, total, near, far, send_sem, recv_sem, part_send, part_recv,
    own_sem,
):
    a, b = lax.axis_index("gx"), lax.axis_index("gy")
    c = lax.axis_index("wa")
    me = a * n_y + b
    offsets = [(i, j) for i in range(n_x) for j in range(n_y) if i or j]
    offsets.sort(key=lambda o: (bool(o[0]) and bool(o[1]), min(o[1], n_y - o[1])))
    peers = [(lax.rem(a + i, n_x), lax.rem(b + j, n_y), c) for i, j in offsets]
    mates = [(a, b, lax.rem(c + k, n_z)) for k in range(1, n_z)]
    barrier = pltpu.get_barrier_semaphore()
    for device in mates + peers:
        pl.semaphore_signal(barrier, inc=1, device_id=device, device_id_type=MESH)
    pl.semaphore_wait(barrier, len(peers) + len(mates))

    def start(src, dst, sems, device):
        copy = pltpu.make_async_remote_copy(
            src_ref=src,
            dst_ref=dst,
            send_sem=sems[0],
            recv_sem=sems[1],
            device_id=device,
            device_id_type=MESH,
        )
        copy.start()
        return copy

    own = pltpu.make_async_copy(squares, near.at[c], own_sem)
    own.start()
    first = [
        start(squares, near.at[c], (part_send.at[k], part_recv.at[k]), device)
        for k, device in enumerate(mates)
    ]
    def blocks_to(k):
        device = peers[k]
        return start(
            send.at[:, device[0] * n_y + device[1]],
            recv.at[:, me],
            (send_sem.at[k], recv_sem.at[k]),
            device,
        )

    ahead = min(3, len(peers))
    copies = [blocks_to(k) for k in range(ahead)]
    own.wait()
    for copy in first:
        copy.wait()
    for k, device in enumerate(peers):
        sem = n_z - 1 + k
        copies.append(start(near, far.at[k], (part_send.at[sem], part_recv.at[sem]), device))
    copies += [blocks_to(k) for k in range(ahead, len(peers))]
    for copy in copies:
        copy.wait()
    total[...] = jnp.sum(near[...], axis=0) + jnp.sum(far[...], axis=(0, 1))


def scale_kernel(every, me, squares, recv, send, out):
    total = jnp.sum(squares[...], keepdims=True)
    scale = 1.0 / jnp.sqrt(total / every + 1e-06)
    own = pl.program_id(0) == me[0]

    @pl.when(own)
    def _():
        out[...] = send[...] * scale[None, None]

    @pl.when(jnp.logical_not(own))
    def _():
        out[...] = recv[...] * scale[None, None]


def local(velocity, lengths, destinations):
    n_x, n_y, n_z = lax.axis_size("gx"), lax.axis_size("gy"), lax.axis_size("wa")
    comps, cells_x, cells_y, cells_z = velocity.shape
    width = BY * BZ
    nblk = cells_x * cells_y * cells_z // width
    writers = n_x * n_y
    capacity = max(2, 2 * nblk // writers)
    f32 = jnp.float32

    smem = pl.BlockSpec(memory_space=pltpu.SMEM)
    vmem = pl.BlockSpec(memory_space=pltpu.VMEM)
    anywhere = pl.BlockSpec(memory_space=pl.ANY)
    slots, y_faces, z_faces = pl.pallas_call(
        functools.partial(faces_kernel, writers, capacity),
        out_shape=(
            jax.ShapeDtypeStruct((nblk // 128, 128), jnp.int32),
            jax.ShapeDtypeStruct((2, 2, cells_x, cells_z), f32),
            jax.ShapeDtypeStruct((2, 2, cells_y, cells_z), f32),
        ),
        name="faces",
    )(destinations.reshape(nblk // 128, 128), velocity)
    halos = pl.pallas_call(
        functools.partial(halo_kernel, (n_x, n_y, n_z)),
        out_shape=jax.ShapeDtypeStruct((6, 2, max(cells_x, cells_y), cells_z), f32),
        in_specs=[anywhere] * 3,
        out_specs=anywhere,
        scratch_shapes=[pltpu.SemaphoreType.DMA((6,)), pltpu.SemaphoreType.DMA((6,))],
        compiler_params=pltpu.CompilerParams(collective_id=1, has_side_effects=True),
        name="halo",
    )(velocity, y_faces, z_faces)

    table = jnp.asarray(split_table())
    outgoing, squares = pl.pallas_call(
        blocks_kernel,
        out_shape=(
            jax.ShapeDtypeStruct((comps * writers * capacity, width), f32),
            jax.ShapeDtypeStruct((8, cells_z), f32),
        ),
        in_specs=[smem, smem] + [vmem] * 3,
        out_specs=(vmem, vmem),
        scratch_shapes=[pltpu.VMEM((comps, nblk, width), f32)],
        compiler_params=pltpu.CompilerParams(vmem_limit_bytes=48 * 2**20),
        name="blocks",
    )(slots.reshape(nblk), lengths.reshape(nblk), velocity, halos, table)
    outgoing = outgoing.reshape(comps, writers, capacity, width)

    arrived, squares = pl.pallas_call(
        functools.partial(exchange_kernel, n_x, n_y, n_z),
        out_shape=(
            jax.ShapeDtypeStruct(outgoing.shape, f32),
            jax.ShapeDtypeStruct(squares.shape, f32),
        ),
        in_specs=[anywhere, vmem],
        out_specs=(anywhere, vmem),
        scratch_shapes=[
            pltpu.VMEM((n_z,) + squares.shape, f32),
            pltpu.VMEM((writers - 1, n_z) + squares.shape, f32),
            pltpu.SemaphoreType.DMA((writers - 1,)),
            pltpu.SemaphoreType.DMA((writers - 1,)),
            pltpu.SemaphoreType.DMA((writers + n_z - 2,)),
            pltpu.SemaphoreType.DMA((writers + n_z - 2,)),
            pltpu.SemaphoreType.DMA,
        ],
        compiler_params=pltpu.CompilerParams(collective_id=0, has_side_effects=True),
        name="exchange",
    )(outgoing, squares)

    every = velocity.size * n_x * n_y * n_z
    me = (lax.axis_index("gx") * n_y + lax.axis_index("gy")).astype(jnp.int32).reshape(1)
    block = (comps, 1, capacity, width)
    received = pl.pallas_call(
        functools.partial(scale_kernel, float(every)),
        grid_spec=pltpu.PrefetchScalarGridSpec(
            num_scalar_prefetch=1,
            grid=(writers,),
            in_specs=[
                pl.BlockSpec((8, cells_z), lambda s, me: (0, 0)),
                pl.BlockSpec(block, lambda s, me: (0, s, 0, 0)),
                pl.BlockSpec(block, lambda s, me: (0, me[0], 0, 0)),
            ],
            out_specs=pl.BlockSpec(block, lambda s, me: (0, s, 0, 0)),
        ),
        out_shape=jax.ShapeDtypeStruct(outgoing.shape, f32),
        name="scale",
    )(me, squares, arrived, outgoing)
    return received.reshape(1, 1, comps, writers, capacity, width)


def solution(mesh):
    return jax.shard_map(
        local,
        mesh=mesh,
        in_specs=(
            P(None, "gx", "gy", "wa"),
            P("gx", "gy", "wa", None),
            P("gx", "gy", "wa", None, None),
        ),
        out_specs=P(("gx", "gy"), "wa", None, None, None, None),
        check_vma=False,
    )
```
